8 devices in a mesh: dp: 2 (over y, z), sp: 4 (over x, core).
Axes of the slice: x: 2, y: 2, z: 1, core: 2. Of those that a mesh axis runs over, the one named last changes fastest.
Arguments:
- x: bfloat16 [4096, 8192], P(('dp', 'sp')), parts along dimension 0
- gain: bfloat16 [8192], replicated
- wq: bfloat16 [8192, 8192], replicated
- wk: bfloat16 [8192, 8192], replicated
- wv: bfloat16 [8192, 8192], replicated
- wo: bfloat16 [8192, 8192], replicated
Outputs:
- output: bfloat16 [4096, 8192], P(('dp', 'sp')), parts along dimension 0
There are 2 independent parts. The reference program is written for one: setup_inputs(seed, part) draws one part's arguments, and reference() takes and returns one part's arrays. A program takes and returns all parts, laid end to end along the dimension named above; an argument that names none is the same for every part.
All inputs are finite; a program needn't handle non-finite values.
Results may differ from the reference program's by a relative error of at most 0.012.
Values are sent between devices in bfloat16 or wider.
A program may use at most 2 GiB of HBM per device.

```python
import jax
import jax.numpy as jnp
from jax import lax

ROWS = 2048
D = 8192
HEADS = 64
KV_HEADS = 64
HEAD = 128
THETA = 10000


def setup_inputs(seed: int = 0, part: int = 0) -> dict:
    kx, kn, kq, kk, kv, ko = jax.random.split(jax.random.key(seed), 6)

    def weights(key, rows, columns):
        return jax.random.normal(key, (rows, columns), jnp.float32) * rows**-0.5

    drawn = {
        "x": jax.random.normal(jax.random.fold_in(kx, part), (ROWS, D), jnp.float32),
        "gain": 1 + 0.1 * jax.random.normal(kn, (D,), jnp.float32),
        "wq": 2 * weights(kq, D, HEADS * HEAD),
        "wk": 2 * weights(kk, D, KV_HEADS * HEAD),
        "wv": 4 * weights(kv, D, KV_HEADS * HEAD),
        "wo": weights(ko, HEADS * HEAD, D),
    }
    return {k: v.astype(jnp.bfloat16) for k, v in drawn.items()}


def normed(x, gain):
    wide = x.astype(jnp.float32)
    scale = lax.rsqrt(jnp.mean(wide * wide, -1, keepdims=True) + 1e-6)
    return (wide * scale * gain.astype(jnp.float32)).astype(jnp.bfloat16)


def turned(t, place, theta):
    half = t.shape[-1] // 2
    angle = place.astype(jnp.float32)[:, None] * theta ** (-jnp.arange(half, dtype=jnp.float32) / half)
    cos, sin = jnp.cos(angle)[:, None], jnp.sin(angle)[:, None]
    a, b = t[..., :half].astype(jnp.float32), t[..., half:].astype(jnp.float32)
    return jnp.concatenate([a * cos - b * sin, b * cos + a * sin], -1).astype(jnp.bfloat16)


def matmul(a, w):
    return jnp.dot(a, w, preferred_element_type=jnp.float32).astype(jnp.bfloat16)


def einsum(form, a, b):
    return jnp.einsum(form, a.astype(jnp.float32), b.astype(jnp.float32))


def attention(q, k, v):
    scores = einsum("tgsd,ugd->gstu", q, k) * q.shape[-1] ** -0.5
    token = jnp.arange(q.shape[0])
    scores = jnp.where(token[:, None] >= token, scores, -jnp.inf)
    weights = jax.nn.softmax(scores, -1).astype(jnp.bfloat16)
    return einsum("gstu,ugd->tgsd", weights, v).astype(jnp.bfloat16)


def reference(x, gain, wq, wk, wv, wo):
    a, place = normed(x, gain), jnp.arange(ROWS)
    q = turned(matmul(a, wq).reshape(ROWS, HEADS, HEAD), place, THETA).reshape(ROWS, KV_HEADS, -1, HEAD)
    k = turned(matmul(a, wk).reshape(ROWS, KV_HEADS, HEAD), place, THETA)
    v = matmul(a, wv).reshape(ROWS, KV_HEADS, HEAD)
    seen = attention(q, k, v).reshape(ROWS, HEADS * HEAD)
    return (x.astype(jnp.float32) + jnp.dot(seen, wo, preferred_element_type=jnp.float32)).astype(jnp.bfloat16)
```

```python
import functools

import jax
import jax.numpy as jnp
from jax import lax
from jax.experimental import pallas as pl
from jax.experimental.pallas import tpu as pltpu

NEG = -1e30
HIDDEN = 2 * NEG
LOG2E = 1.4426950408889634


def _dot(a, b, ca, cb):
    return lax.dot_general(a, b, (((ca,), (cb,)), ((), ())), preferred_element_type=jnp.float32)


from jax.sharding import PartitionSpec as P

HEAD = 128
THETA = 10000
LIMIT = 60 * 2**20


def normed(x, gain):
    wide = x.astype(jnp.float32)
    scale = lax.rsqrt(jnp.mean(wide * wide, -1, keepdims=True) + 1e-6)
    return (wide * scale * gain.astype(jnp.float32)).astype(jnp.bfloat16)


def tables(tokens):
    half = HEAD // 2
    angle = jnp.arange(tokens, dtype=jnp.float32)[:, None] * THETA ** (-jnp.arange(half, dtype=jnp.float32) / half)
    cos, sin = jnp.cos(angle), jnp.sin(angle)
    return jnp.concatenate([cos, cos], -1), jnp.concatenate([-sin, sin], -1)


def _project(at, a_ref, cos_ref, sin_ref, wq, wk, wv, *rest, bn, nb):
    out_ref, buf, sem = rest[-3:]
    step, heads = pl.program_id(0), bn // HEAD
    first = at[0] * (nb * bn)

    def start(s):
        columns = pl.ds(pl.multiple_of(first + lax.rem(s, nb) * bn, bn), bn)
        for i, w in enumerate((wq, wk, wv)):

            @pl.when(s // nb == i)
            def _():
                pltpu.make_async_copy(w.at[:, columns], buf.at[lax.rem(s, 2)], sem.at[lax.rem(s, 2)]).start()

    @pl.when(step == 0)
    def _():
        start(0)

    @pl.when(step + 1 < 3 * nb)
    def _():
        start(step + 1)

    slot = lax.rem(step, 2)
    pltpu.make_async_copy(wq.at[:, pl.ds(0, bn)], buf.at[slot], sem.at[slot]).wait()
    got = jnp.dot(a_ref[...], buf[slot], preferred_element_type=jnp.float32).astype(jnp.bfloat16)

    @pl.when(step < 2 * nb)
    def _():
        for h in range(heads):
            t = got[:, h * HEAD : (h + 1) * HEAD].astype(jnp.float32)
            out_ref[h] = (t * cos_ref[...] + pltpu.roll(t, HEAD // 2, 1) * sin_ref[...]).astype(jnp.bfloat16)

    @pl.when(step >= 2 * nb)
    def _():
        for h in range(heads):
            out_ref[h] = got[:, h * HEAD : (h + 1) * HEAD]


def project(at, a, cos, sin, wq, wk, wv, into, tokens, heads, bn=256):
    m, d = a.shape
    nb = heads * HEAD // bn
    hbm = pl.BlockSpec(memory_space=pl.ANY)
    rows = pl.BlockSpec((m, HEAD), lambda s, at: (at[1], 0))
    given = [a, cos, sin, wq, wk, wv] + ([] if into is None else [into])
    return pl.pallas_call(
        functools.partial(_project, bn=bn, nb=nb),
        grid_spec=pltpu.PrefetchScalarGridSpec(
            num_scalar_prefetch=1,
            grid=(3 * nb,),
            in_specs=[pl.BlockSpec((m, d), lambda s, at: (0, 0), pipeline_mode=pl.Buffered(1)), rows, rows] + [hbm] * (len(given) - 3),
            out_specs=pl.BlockSpec((bn // HEAD, m, HEAD), lambda s, at: (s, at[1], 0)),
            scratch_shapes=[pltpu.VMEM((2, d, bn), jnp.bfloat16), pltpu.SemaphoreType.DMA((2,))],
        ),
        out_shape=jax.ShapeDtypeStruct((3 * heads, tokens, HEAD), jnp.bfloat16),
        input_output_aliases={} if into is None else {7: 0},
        compiler_params=pltpu.CompilerParams(dimension_semantics=("arbitrary",), vmem_limit_bytes=LIMIT),
        cost_estimate=pl.CostEstimate(flops=6 * m * d * heads * HEAD, bytes_accessed=6 * d * heads * HEAD, transcendentals=0),
    )(at, *given)


def _attend_rows(at, q_ref, k_ref, v_ref, o_ref, top_s, mix_s, *, bk, scale):
    hb, bq, d = q_ref.shape
    e = scale * LOG2E
    b = at[0]
    top_s[...] = jnp.full(top_s.shape, NEG, jnp.float32)
    mix_s[...] = jnp.zeros(mix_s.shape, jnp.float32)
    ones = jnp.ones((8, bk), jnp.bfloat16)

    def block(j, masked):
        here = pl.ds(pl.multiple_of(j * bk, bk), bk)
        scores = [_dot(k_ref[i, here, :], q_ref[i], 1, 1) for i in range(hb)]
        weights, keeps = [], []
        if masked:
            gap = lax.broadcasted_iota(jnp.int32, (bk, bq), 1) - lax.broadcasted_iota(jnp.int32, (bk, bq), 0)
            ok = gap >= j * bk - b * bq
        for i, s in enumerate(scores):
            if masked:
                s = jnp.where(ok, s, HIDDEN)
            old = top_s[i : i + 1, :]
            top = jnp.maximum(old, s.max(axis=0, keepdims=True))
            top_s[i : i + 1, :] = top
            weights.append(jnp.exp2((s - top) * e).astype(jnp.bfloat16))
            keeps.append(jnp.exp2((old - top) * e))
        for i, (p, keep) in enumerate(zip(weights, keeps)):
            values = jnp.concatenate([v_ref[i, here, :].T, ones], axis=0)
            mix_s[i] = mix_s[i] * keep + _dot(values, p, 1, 0)

    per = bq // bk
    lax.fori_loop(0, b * per, lambda j, _: block(j, False), None)
    lax.fori_loop(b * per, (b + 1) * per, lambda j, _: block(j, True), None)
    for i in range(hb):
        o_ref[:, i * d : (i + 1) * d] = (mix_s[i, :d, :] * (1 / mix_s[i, d : d + 1, :])).T.astype(o_ref.dtype)


def attend_rows(b, qkv, bq=512, hb=4, bk=512):
    heads, tokens = qkv.shape[0] // 3, qkv.shape[1]
    n = heads // hb
    return pl.pallas_call(
        functools.partial(_attend_rows, bk=bk, scale=HEAD**-0.5),
        grid_spec=pltpu.PrefetchScalarGridSpec(
            num_scalar_prefetch=1,
            grid=(n,),
            in_specs=[
                pl.BlockSpec((hb, bq, HEAD), lambda h, at: (h, at[0], 0)),
                pl.BlockSpec((hb, tokens, HEAD), lambda h, at: (n + h, 0, 0)),
                pl.BlockSpec((hb, tokens, HEAD), lambda h, at: (2 * n + h, 0, 0)),
            ],
            out_specs=pl.BlockSpec((bq, hb * HEAD), lambda h, at: (0, h)),
            scratch_shapes=[pltpu.VMEM((hb, bq), jnp.float32), pltpu.VMEM((hb, HEAD + 8, bq), jnp.float32)],
        ),
        out_shape=jax.ShapeDtypeStruct((bq, heads * HEAD), jnp.bfloat16),
        compiler_params=pltpu.CompilerParams(dimension_semantics=("arbitrary",), vmem_limit_bytes=LIMIT),
        cost_estimate=pl.CostEstimate(flops=16 * heads * bq * tokens * HEAD // 4, bytes_accessed=4 * heads * tokens * HEAD, transcendentals=0),
    )(b, qkv, qkv, qkv)


def _output(at, s0_ref, s1_ref, w0_ref, w1_ref, *rest, last):
    total = jnp.dot(s0_ref[...], w0_ref[...], preferred_element_type=jnp.float32)
    total += jnp.dot(s1_ref[...], w1_ref[...], preferred_element_type=jnp.float32)
    if last:
        part_ref, x_ref, o_ref = rest
        o_ref[...] = (x_ref[...].astype(jnp.float32) + (part_ref[...] + total)).astype(jnp.bfloat16)
    else:
        rest[0][...] = total


def output(at, s0, s1, wo, part=None, x=None, bn=512):
    m, depth = s0.shape
    n = wo.shape[1]
    whole = pl.BlockSpec((m, depth), lambda j, at: (0, 0), pipeline_mode=pl.Buffered(1))
    run = lambda i: pl.BlockSpec((depth, bn), lambda j, at: (at[i], j))
    block = pl.BlockSpec((m, bn), lambda j, at: (0, j))
    last = part is not None
    return pl.pallas_call(
        functools.partial(_output, last=last),
        grid_spec=pltpu.PrefetchScalarGridSpec(
            num_scalar_prefetch=1,
            grid=(n // bn,),
            in_specs=[whole, whole, run(0), run(1)] + ([block, block] if last else []),
            out_specs=block,
        ),
        out_shape=jax.ShapeDtypeStruct((m, n), jnp.bfloat16 if last else jnp.float32),
        compiler_params=pltpu.CompilerParams(dimension_semantics=("arbitrary",), vmem_limit_bytes=LIMIT),
        cost_estimate=pl.CostEstimate(flops=4 * m * depth * n, bytes_accessed=4 * depth * n, transcendentals=0),
    )(at, s0, s1, wo, wo, *([part, x] if last else []))


def solution(mesh):
    n = mesh.shape["sp"]

    def swap(t, bits):
        return lax.ppermute(t, "sp", [(i, i ^ bits) for i in range(n)])

    def step(x, gain, wq, wk, wv, wo):
        own, tokens = x.shape[0], x.shape[0] * n
        heads = wq.shape[1] // HEAD // n
        me = lax.axis_index("sp").astype(jnp.int32)
        core, chip = me & 1, me & 2
        a = normed(x, gain)
        cos, sin = tables(tokens)
        beside = swap(a, 1)
        half = own // 2
        zero, one = jnp.where(core == 0, a, beside), jnp.where(core == 0, beside, a)
        far = []
        for rows in (zero, one):
            got = swap(lax.dynamic_slice_in_dim(rows, core * half, half, 0), 2)
            other = swap(got, 1)
            far.append(jnp.where(core == 0, jnp.concatenate([got, other]), jnp.concatenate([other, got])))

        def proj(rows, block, into):
            return project(jnp.stack([me, block]), rows, cos, sin, wq, wk, wv, into, tokens, heads)

        qkv = proj(a, me, None)
        qkv = proj(beside, me ^ 1, qkv)
        qkv = proj(far[0], chip ^ 2, qkv)
        qkv = proj(far[1], (chip ^ 2) + 1, qkv)
        seen = {j: attend_rows((me ^ j)[None], qkv) for j in (2, 3, 1, 0)}
        seen = {j: s if j == 0 else swap(s, j) for j, s in seen.items()}
        part = output(jnp.stack([me, me ^ 1]), seen[0], seen[1], wo)
        return output(jnp.stack([me ^ 2, me ^ 3]), seen[2], seen[3], wo, part, x)

    tokens, whole = P(("dp", "sp"), None), P(None, None)
    return jax.shard_map(
        step,
        mesh=mesh,
        in_specs=(tokens, P(None), whole, whole, whole, whole),
        out_specs=tokens,
        check_vma=False,
    )
```

```python
import functools

import jax
import jax.numpy as jnp
from jax import lax
from jax.experimental import pallas as pl
from jax.experimental.pallas import tpu as pltpu

NEG = -1e30
HIDDEN = 2 * NEG
LOG2E = 1.4426950408889634


def _dot(a, b, ca, cb):
    return lax.dot_general(a, b, (((ca,), (cb,)), ((), ())), preferred_element_type=jnp.float32)


from jax.sharding import PartitionSpec as P

HEAD = 128
THETA = 10000
LIMIT = 60 * 2**20
DEPTHS = 4
DIAG = 2
HBM = pl.BlockSpec(memory_space=pl.ANY)


def _params():
    return pltpu.CompilerParams(dimension_semantics=("arbitrary",), vmem_limit_bytes=LIMIT)


def tables(tokens):
    half = HEAD // 2
    angle = jnp.arange(tokens, dtype=jnp.float32)[:, None] * THETA ** (-jnp.arange(half, dtype=jnp.float32) / half)
    cos, sin = jnp.cos(angle), jnp.sin(angle)
    return jnp.concatenate([cos, cos], -1), jnp.concatenate([-sin, sin], -1)


def _norm(x_ref, gain_ref, o_ref):
    wide = x_ref[...].astype(jnp.float32)
    scale = lax.rsqrt(jnp.mean(wide * wide, -1, keepdims=True) + 1e-6)
    o_ref[...] = (wide * scale * gain_ref[...][None].astype(jnp.float32)).astype(jnp.bfloat16)


def norm(x, gain, rows=128):
    m, d = x.shape
    block = pl.BlockSpec((rows, d), lambda i: (i, 0))
    return pl.pallas_call(
        _norm,
        grid=(m // rows,),
        in_specs=[block, pl.BlockSpec((d,), lambda i: (0,))],
        out_specs=block,
        out_shape=jax.ShapeDtypeStruct(x.shape, jnp.bfloat16),
        compiler_params=_params(),
        cost_estimate=pl.CostEstimate(flops=5 * m * d, bytes_accessed=4 * m * d, transcendentals=0),
    )(x, gain)


def _project(at, *refs, count, place, kinds, bn, nb):
    pieces, (cos_ref, sin_ref), weights = refs[:count], refs[count : count + 2], refs[count + 2 : count + 2 + len(kinds)]
    out_ref, rows, buf, acc, sem, first_sem, row_sem = refs[-7:]
    step, heads = pl.program_id(0), bn // HEAD
    core, first = lax.rem(at[0], 2), at[0] * (nb * bn)
    m, steps = pieces[0].shape[0], len(kinds) * nb
    plain = kinds.index(2) * nb if 2 in kinds else steps
    deep = rows.shape[1] // DEPTHS

    def depth(c):
        return pl.ds(pl.multiple_of(c * deep, deep), deep)

    def start(s):
        for i, w in enumerate(weights):

            @pl.when((s >= i * nb) & (s < (i + 1) * nb))
            def _():
                columns = pl.ds(pl.multiple_of(first + (s - i * nb) * bn, bn), bn)
                pltpu.make_async_copy(w.at[:, columns], buf.at[lax.rem(s, 2)], sem.at[lax.rem(s, 2)]).start()

    def finish(got):
        for h in range(heads):
            t = got[:, h * HEAD : (h + 1) * HEAD].astype(jnp.float32)
            turned = t * cos_ref[...] + pltpu.roll(t, HEAD // 2, 1) * sin_ref[...]
            out_ref[h] = jnp.where(step < plain, turned, t).astype(jnp.bfloat16)

    @pl.when(step == 0)
    def _():
        columns = pl.ds(pl.multiple_of(first, bn), bn)
        for c in range(DEPTHS):
            for k in (0, 1):

                @pl.when(core == k)
                def _():
                    for p, to in place[k]:
                        pltpu.make_async_copy(pieces[p].at[:, depth(c)], rows.at[pl.ds(to, m), depth(c)], row_sem.at[c, to // m]).start()

            pltpu.make_async_copy(weights[0].at[depth(c), columns], buf.at[0, depth(c)], first_sem.at[c]).start()
        start(1)
        acc[...] = jnp.zeros_like(acc)

        def add(c, _):
            for i in range(rows.shape[0] // m):
                pltpu.make_async_copy(pieces[0].at[:, depth(c)], rows.at[pl.ds(i * m, m), depth(c)], row_sem.at[c, i]).wait()
            pltpu.make_async_copy(weights[0].at[depth(c), columns], buf.at[0, depth(c)], first_sem.at[c]).wait()
            acc[...] += jnp.dot(rows[:, depth(c)], buf[0, depth(c), :], preferred_element_type=jnp.float32)

        lax.fori_loop(0, DEPTHS, add, None)
        finish(acc[...].astype(jnp.bfloat16))

    @pl.when(step > 0)
    def _():
        slot = lax.rem(step, 2)

        @pl.when(step + 1 < steps)
        def _():
            start(step + 1)

        pltpu.make_async_copy(weights[0].at[:, pl.ds(0, bn)], buf.at[slot], sem.at[slot]).wait()
        finish(jnp.dot(rows[...], buf[slot], preferred_element_type=jnp.float32).astype(jnp.bfloat16))


def project(me, pieces, place, block, cos, sin, weights, kinds, into, tokens, heads, bn):
    m, d = pieces[0].shape
    nb = heads * HEAD // bn
    total = m * len(place[0])
    rows = pl.BlockSpec((total, HEAD), lambda s, at: (block(at[0]), 0))
    given = [*pieces, cos, sin, *(weights[k] for k in kinds)] + ([] if into is None else [into])
    specs = [HBM] * len(pieces) + [rows, rows] + [HBM] * (len(kinds) + (into is not None))
    return pl.pallas_call(
        functools.partial(_project, count=len(pieces), place=place, kinds=kinds, bn=bn, nb=nb),
        grid_spec=pltpu.PrefetchScalarGridSpec(
            num_scalar_prefetch=1,
            grid=(len(kinds) * nb,),
            in_specs=specs,
            out_specs=pl.BlockSpec((bn // HEAD, total, HEAD), lambda s, at: (s + kinds[0] * nb, block(at[0]), 0)),
            scratch_shapes=[
                pltpu.VMEM((total, d), jnp.bfloat16),
                pltpu.VMEM((2, d, bn), jnp.bfloat16),
                pltpu.VMEM((total, bn), jnp.float32),
                pltpu.SemaphoreType.DMA((2,)),
                pltpu.SemaphoreType.DMA((DEPTHS,)),
                pltpu.SemaphoreType.DMA((DEPTHS, len(place[0]))),
            ],
        ),
        out_shape=jax.ShapeDtypeStruct((3 * heads, tokens, HEAD), jnp.bfloat16),
        input_output_aliases={} if into is None else {len(given): 0},
        compiler_params=_params(),
        cost_estimate=pl.CostEstimate(flops=2 * len(kinds) * total * d * heads * HEAD, bytes_accessed=2 * len(kinds) * d * heads * HEAD, transcendentals=0),
    )(me, *given)


def _pick(at, items, i, field):
    got = [jnp.where(lax.div(at[0], 2) == 0, a[field], b[field]) for a, b in items]
    value = got[-1]
    for n in range(len(got) - 2, -1, -1):
        value = jnp.where(i == n, got[n], value)
    return value


def _work(at, q_ref, k_ref, v_ref, *rest, items, kinds, scale, carry, bq):
    top_s, mix_s = rest[-2:]
    state_in, outs = (rest[0], rest[1:-2]) if carry is not None else (None, rest[:-2])
    hb, _, d = q_ref.shape
    e = scale * LOG2E

    def one_item(item):
        query, lo, hi, goes_on = (_pick(at, items, item, f) for f in range(4))

        @pl.when(goes_on == 0)
        def _():
            top_s[...] = jnp.full(top_s.shape, NEG, jnp.float32)
            mix_s[...] = jnp.zeros(mix_s.shape, jnp.float32)

        if carry is not None:

            @pl.when(goes_on == 1)
            def _():
                for i in range(hb):
                    top_s[i : i + 1, :] = state_in[0, i, d + 1 : d + 2, :]
                    mix_s[i] = state_in[0, i]

        def block(first, keys, at_q, masked):
            here = pl.ds(pl.multiple_of(first, keys), keys)
            there = pl.ds(pl.multiple_of(query * bq + at_q, keys), bq - at_q)
            cols = slice(at_q, bq)
            ones = jnp.ones((8, keys), jnp.bfloat16)
            scores = [_dot(k_ref[i, here, :], q_ref[i, there, :], 1, 1) for i in range(hb)]
            weights, keeps = [], []
            if masked:
                ok = lax.broadcasted_iota(jnp.int32, scores[0].shape, 1) >= lax.broadcasted_iota(jnp.int32, scores[0].shape, 0)
            for i, s in enumerate(scores):
                if masked:
                    s = jnp.where(ok, s, HIDDEN)
                old = top_s[i : i + 1, cols]
                top = jnp.maximum(old, s.max(axis=0, keepdims=True))
                top_s[i : i + 1, cols] = top
                weights.append(jnp.exp2((s - top) * e).astype(jnp.bfloat16))
                keeps.append(jnp.exp2((old - top) * e))
            for i, (p, keep) in enumerate(zip(weights, keeps)):
                values = jnp.concatenate([v_ref[i, here, :].T, ones], axis=0)
                mix_s[i, :, cols] = mix_s[i, :, cols] * keep + _dot(values, p, 1, 0)

        lax.fori_loop(lo, jnp.minimum(hi, query), lambda j, _: block(j * bq, bq, 0, False), None)

        @pl.when(hi == query + 1)
        def _():
            step = bq // DIAG
            for n in range(DIAG):
                block(query * bq + n * step, step, n * step, True)

        for n, kind in enumerate(kinds):

            @pl.when(item == n)
            def _():
                for i in range(hb):
                    if kind == "state":
                        at_state = n - kinds.count("out")
                        outs[-1][at_state, i] = mix_s[i]
                        outs[-1][at_state, i, d + 1 : d + 2, :] = top_s[i : i + 1, :]
                    else:
                        outs[n][:, i * d : (i + 1) * d] = (mix_s[i, :d, :] * (1 / mix_s[i, d : d + 1, :])).T.astype(jnp.bfloat16)

    if len(items) == 1:
        one_item(0)
    else:
        lax.fori_loop(0, len(items), lambda item, _: one_item(item), None)


def work(me, qkv, items, kinds, state=None, carry=None, bq=512, hb=4):
    heads, tokens = qkv.shape[0] // 3, qkv.shape[1]
    n = heads // hb
    states, done = kinds.count("state"), kinds.count("out")
    run = lambda i: pl.BlockSpec((hb, tokens, HEAD), lambda h, at: (i * n + h, 0, 0))
    specs = [run(0), run(1), run(2)]
    if carry is not None:
        specs.append(pl.BlockSpec((1, hb, HEAD + 8, bq), lambda h, at: (carry, h, 0, 0)))
    outs = [(pl.BlockSpec((bq, hb * HEAD), lambda h, at: (0, h)), jax.ShapeDtypeStruct((bq, heads * HEAD), jnp.bfloat16))] * done
    if states:
        outs.append((pl.BlockSpec((states, hb, HEAD + 8, bq), lambda h, at: (0, h, 0, 0)), jax.ShapeDtypeStruct((states, heads, HEAD + 8, bq), jnp.float32)))
    pairs = max(sum(i[c][2] - i[c][1] for i in items) for c in (0, 1))
    return pl.pallas_call(
        functools.partial(_work, items=items, kinds=kinds, scale=HEAD**-0.5, carry=carry, bq=bq),
        grid_spec=pltpu.PrefetchScalarGridSpec(
            num_scalar_prefetch=1,
            grid=(n,),
            in_specs=specs,
            out_specs=[o[0] for o in outs],
            scratch_shapes=[pltpu.VMEM((hb, bq), jnp.float32), pltpu.VMEM((hb, HEAD + 8, bq), jnp.float32)],
        ),
        out_shape=[o[1] for o in outs],
        compiler_params=_params(),
        cost_estimate=pl.CostEstimate(flops=8 * pairs * heads * bq * bq * HEAD, bytes_accessed=4 * heads * tokens * HEAD, transcendentals=0),
    )(me, qkv, qkv, qkv, *([state] if carry is not None else []))


def _output(at, *refs, last):
    sources, w_ref, rest = refs[:4], refs[4], refs[5:]
    o_ref, rows, sem = rest[-3:]
    depth = sources[0].shape[1]

    @pl.when(pl.program_id(0) == 0)
    def _():
        for c in (0, 1):

            @pl.when(lax.rem(at[0], 2) == c)
            def _():
                for i in (0, 1):
                    to = rows.at[:, pl.ds((c ^ i) * depth, depth)]
                    pltpu.make_async_copy(sources[2 * c + i], to, sem.at[i]).start()

        for i in (0, 1):
            pltpu.make_async_copy(sources[i], rows.at[:, pl.ds(0, depth)], sem.at[i]).wait()

    total = jnp.dot(rows[...], w_ref[...], preferred_element_type=jnp.float32)
    if last:
        part_ref, x_ref = rest[:2]
        o_ref[...] = (x_ref[...].astype(jnp.float32) + (part_ref[...] + total)).astype(jnp.bfloat16)
    else:
        o_ref[...] = total


def output(me, zero, one, other, wo, part=None, x=None, bn=512):
    m, depth = zero[0].shape
    n = wo.shape[1]
    block = pl.BlockSpec((m, bn), lambda j, at: (0, j))
    last = part is not None
    return pl.pallas_call(
        functools.partial(_output, last=last),
        grid_spec=pltpu.PrefetchScalarGridSpec(
            num_scalar_prefetch=1,
            grid=(n // bn,),
            in_specs=[HBM] * 4 + [pl.BlockSpec((2 * depth, bn), lambda j, at: (at[0] // 2 ^ other, j))] + ([block, block] if last else []),
            out_specs=block,
            scratch_shapes=[pltpu.VMEM((m, 2 * depth), jnp.bfloat16), pltpu.SemaphoreType.DMA((2,))],
        ),
        out_shape=jax.ShapeDtypeStruct((m, n), jnp.bfloat16 if last else jnp.float32),
        compiler_params=_params(),
        cost_estimate=pl.CostEstimate(flops=4 * m * depth * n, bytes_accessed=4 * depth * n, transcendentals=0),
    )(me, *zero, *one, wo, *([part, x] if last else []))


def solution(mesh):
    n = mesh.shape["sp"]
    send = lambda t, *pairs: lax.ppermute(t, "sp", pairs)

    def step(x, gain, wq, wk, wv, wo):
        own, tokens = x.shape[0], x.shape[0] * n
        heads = wq.shape[1] // HEAD // n
        me = lax.axis_index("sp").astype(jnp.int32)[None]
        cos, sin = tables(tokens)

        def proj(pieces, place, block, kinds, into, bn=512):
            return project(me, pieces, place, block, cos, sin, (wq, wk, wv), kinds, into, tokens, heads, bn)

        a = norm(x, gain)
        near = send(a, (0, 1), (1, 0), (2, 3), (3, 2))
        zero = send(a, (0, 2), (2, 0))
        places = [[(0, 0), (1, own)], [(1, 0), (0, own)]]
        qkv = proj([a, near], places, lambda d: d // 2, (0, 1), None, 256)
        qkv, zero = lax.optimization_barrier((qkv, zero))
        one = send(lax.optimization_barrier((a, qkv))[0], (1, 3), (3, 1))
        zero_on = send(zero, (0, 1), (2, 3))
        qkv = proj([a, near], places, lambda d: d // 2, (2,), qkv, 256)
        places = [[(0, 0)], [(1, 0)]]
        qkv = proj([zero, zero_on], places, lambda d: (d // 2 ^ 1) * 2, (0, 1, 2), qkv)
        qkv, one = lax.optimization_barrier((qkv, one))
        one_on = send(one, (1, 0), (3, 2))
        x0, state = work(me, qkv, [((2, 0, 3, 0), (0, 0, 1, 0)), ((2, 0, 0, 0), (2, 2, 3, 0)), ((2, 0, 0, 0), (3, 2, 4, 0))], ["out", "state", "state"])
        x0 = send(x0, (0, 2), (2, 0)), send(x0, (1, 2), (3, 0))
        qkv = proj([one_on, one], places, lambda d: (d // 2 ^ 1) * 2 + 1, (0, 1, 2), qkv)
        x1, l0 = work(me, qkv, [((3, 0, 4, 0), (1, 0, 2, 0)), ((0, 0, 1, 0), (2, 0, 2, 1))], ["out", "out"], state, 0)
        x1 = send(x1, (1, 3), (3, 1)), send(x1, (0, 3), (2, 1))
        (l1,) = work(me, qkv, [((1, 0, 2, 0), (3, 0, 2, 1))], ["out"], state, 1)
        l0 = l0, send(l0, (1, 0), (3, 2))
        l1 = l1, send(l1, (0, 1), (2, 3))
        part = output(me, l0, l1, 0, wo)
        return output(me, x0, x1, 1, wo, part, x)

    tokens, whole = P(("dp", "sp"), None), P(None, None)
    step = jax.shard_map(step, mesh=mesh, in_specs=(tokens, P(None), whole, whole, whole, whole), out_specs=tokens, check_vma=False)
    return step
```

```python
import functools

import jax
import jax.numpy as jnp
from jax import lax
from jax.experimental import pallas as pl
from jax.experimental.pallas import tpu as pltpu

NEG = -1e30
HIDDEN = 2 * NEG
LOG2E = 1.4426950408889634


def _dot(a, b, ca, cb):
    return lax.dot_general(a, b, (((ca,), (cb,)), ((), ())), preferred_element_type=jnp.float32)


from jax.sharding import PartitionSpec as P

HEAD = 128
THETA = 10000
LIMIT = 34 * 2**20
DEPTHS = 4
DIAG = 2
HBM = pl.BlockSpec(memory_space=pl.ANY)


def _params():
    return pltpu.CompilerParams(dimension_semantics=("arbitrary",), vmem_limit_bytes=LIMIT)


def tables(tokens):
    half = HEAD // 2
    angle = jnp.arange(tokens, dtype=jnp.float32)[:, None] * THETA ** (-jnp.arange(half, dtype=jnp.float32) / half)
    cos, sin = jnp.cos(angle), jnp.sin(angle)
    return jnp.concatenate([cos, cos], -1), jnp.concatenate([-sin, sin], -1)


def _norm(x_ref, gain_ref, o_ref):
    wide = x_ref[...].astype(jnp.float32)
    scale = lax.rsqrt(jnp.mean(wide * wide, -1, keepdims=True) + 1e-6)
    o_ref[...] = (wide * scale * gain_ref[...][None].astype(jnp.float32)).astype(jnp.bfloat16)


def norm(x, gain, rows=128):
    m, d = x.shape
    block = pl.BlockSpec((rows, d), lambda i: (i, 0))
    return pl.pallas_call(
        _norm,
        grid=(m // rows,),
        in_specs=[block, pl.BlockSpec((d,), lambda i: (0,))],
        out_specs=block,
        out_shape=jax.ShapeDtypeStruct(x.shape, jnp.bfloat16),
        compiler_params=_params(),
        cost_estimate=pl.CostEstimate(flops=5 * m * d, bytes_accessed=4 * m * d, transcendentals=0),
    )(x, gain)


def _project(at, *refs, count, place, kinds, bn, nb):
    pieces, (cos_ref, sin_ref), weights = refs[:count], refs[count : count + 2], refs[count + 2 : count + 2 + len(kinds)]
    out_ref, rows, buf, acc, sem, first_sem, row_sem = refs[-7:]
    step, heads = pl.program_id(0), bn // HEAD
    core, first = lax.rem(at[0], 2), at[0] * (nb * bn)
    m, steps = pieces[0].shape[0], len(kinds) * nb
    plain = kinds.index(2) * nb if 2 in kinds else steps
    deep = rows.shape[1] // DEPTHS

    def depth(c):
        return pl.ds(pl.multiple_of(c * deep, deep), deep)

    def start(s):
        for i, w in enumerate(weights):

            @pl.when((s >= i * nb) & (s < (i + 1) * nb))
            def _():
                columns = pl.ds(pl.multiple_of(first + (s - i * nb) * bn, bn), bn)
                pltpu.make_async_copy(w.at[:, columns], buf.at[lax.rem(s, 2)], sem.at[lax.rem(s, 2)]).start()

    def finish(got):
        for h in range(heads):
            t = got[:, h * HEAD : (h + 1) * HEAD].astype(jnp.float32)
            turned = t * cos_ref[...] + pltpu.roll(t, HEAD // 2, 1) * sin_ref[...]
            out_ref[h] = jnp.where(step < plain, turned, t).astype(jnp.bfloat16)

    @pl.when(step == 0)
    def _():
        columns = pl.ds(pl.multiple_of(first, bn), bn)
        for c in range(DEPTHS):
            for k in (0, 1):

                @pl.when(core == k)
                def _():
                    for p, to in place[k]:
                        pltpu.make_async_copy(pieces[p].at[:, depth(c)], rows.at[pl.ds(to, m), depth(c)], row_sem.at[c, to // m]).start()

            pltpu.make_async_copy(weights[0].at[depth(c), columns], buf.at[0, depth(c)], first_sem.at[c]).start()
        start(1)
        acc[...] = jnp.zeros_like(acc)

        def add(c, _):
            for i in range(rows.shape[0] // m):
                pltpu.make_async_copy(pieces[0].at[:, depth(c)], rows.at[pl.ds(i * m, m), depth(c)], row_sem.at[c, i]).wait()
            pltpu.make_async_copy(weights[0].at[depth(c), columns], buf.at[0, depth(c)], first_sem.at[c]).wait()
            acc[...] += jnp.dot(rows[:, depth(c)], buf[0, depth(c), :], preferred_element_type=jnp.float32)

        lax.fori_loop(0, DEPTHS, add, None)
        finish(acc[...].astype(jnp.bfloat16))

    @pl.when(step > 0)
    def _():
        slot = lax.rem(step, 2)

        @pl.when(step + 1 < steps)
        def _():
            start(step + 1)

        pltpu.make_async_copy(weights[0].at[:, pl.ds(0, bn)], buf.at[slot], sem.at[slot]).wait()
        finish(jnp.dot(rows[...], buf[slot], preferred_element_type=jnp.float32).astype(jnp.bfloat16))


def project(me, pieces, place, block, cos, sin, weights, kinds, into, tokens, heads, bn):
    m, d = pieces[0].shape
    nb = heads * HEAD // bn
    total = m * len(place[0])
    rows = pl.BlockSpec((total, HEAD), lambda s, at: (block(at[0]), 0))
    given = [*pieces, cos, sin, *(weights[k] for k in kinds)] + ([] if into is None else [into])
    specs = [HBM] * len(pieces) + [rows, rows] + [HBM] * (len(kinds) + (into is not None))
    return pl.pallas_call(
        functools.partial(_project, count=len(pieces), place=place, kinds=kinds, bn=bn, nb=nb),
        grid_spec=pltpu.PrefetchScalarGridSpec(
            num_scalar_prefetch=1,
            grid=(len(kinds) * nb,),
            in_specs=specs,
            out_specs=pl.BlockSpec((bn // HEAD, total, HEAD), lambda s, at: (s + kinds[0] * nb, block(at[0]), 0)),
            scratch_shapes=[
                pltpu.VMEM((total, d), jnp.bfloat16),
                pltpu.VMEM((2, d, bn), jnp.bfloat16),
                pltpu.VMEM((total, bn), jnp.float32),
                pltpu.SemaphoreType.DMA((2,)),
                pltpu.SemaphoreType.DMA((DEPTHS,)),
                pltpu.SemaphoreType.DMA((DEPTHS, len(place[0]))),
            ],
        ),
        out_shape=jax.ShapeDtypeStruct((3 * heads, tokens, HEAD), jnp.bfloat16),
        input_output_aliases={} if into is None else {len(given): 0},
        compiler_params=_params(),
        cost_estimate=pl.CostEstimate(flops=2 * len(kinds) * total * d * heads * HEAD, bytes_accessed=2 * len(kinds) * d * heads * HEAD, transcendentals=0),
    )(me, *given)


def _pick(at, items, i, field):
    got = [jnp.where(lax.div(at[0], 2) == 0, a[field], b[field]) for a, b in items]
    value = got[-1]
    for n in range(len(got) - 2, -1, -1):
        value = jnp.where(i == n, got[n], value)
    return value


def _work(at, q_ref, k_ref, v_ref, *rest, items, kinds, scale, given, bq):
    top_s, mix_s = rest[-2:]
    state_in, outs = (rest[0], rest[1:-2]) if given else (None, rest[:-2])
    hb, _, d = q_ref.shape
    e = scale * LOG2E

    def one_item(item):
        query, lo, hi, goes_on = (_pick(at, items, item, f) for f in range(4))

        @pl.when(goes_on == 0)
        def _():
            top_s[...] = jnp.full(top_s.shape, NEG, jnp.float32)
            mix_s[...] = jnp.zeros(mix_s.shape, jnp.float32)

        if given:

            @pl.when(goes_on == 1)
            def _():
                for i in range(hb):
                    top_s[i : i + 1, :] = state_in[0, i, d + 1 : d + 2, :]
                    mix_s[i] = state_in[0, i]

        def block(first, pieces, masked):
            pieces = [(i, slice(a, b), keys) for i in range(hb) for a, b, keys in pieces]
            here = lambda keys: pl.ds(pl.multiple_of(first, bq), keys)
            there = lambda cols: pl.ds(pl.multiple_of(query * bq + cols.start, cols.stop - cols.start), cols.stop - cols.start)
            scores = [_dot(k_ref[i, here(keys), :], q_ref[i, there(cols), :], 1, 1) for i, cols, keys in pieces]
            weights, keeps = [], []
            for (i, cols, _), s in zip(pieces, scores):
                if masked:
                    s = jnp.where(lax.broadcasted_iota(jnp.int32, s.shape, 1) + cols.start >= lax.broadcasted_iota(jnp.int32, s.shape, 0), s, HIDDEN)
                old = top_s[i : i + 1, cols]
                top = jnp.maximum(old, s.max(axis=0, keepdims=True))
                top_s[i : i + 1, cols] = top
                weights.append(jnp.exp2((s - top) * e).astype(jnp.bfloat16))
                keeps.append(jnp.exp2((old - top) * e))
            for (i, cols, keys), p, keep in zip(pieces, weights, keeps):
                values = jnp.concatenate([v_ref[i, here(keys), :].T, jnp.ones((8, keys), jnp.bfloat16)], axis=0)
                mix_s[i, :, cols] = mix_s[i, :, cols] * keep + _dot(values, p, 1, 0)

        lax.fori_loop(lo, jnp.minimum(hi, query), lambda j, _: block(j * bq, [(0, bq, bq)], False), None)

        @pl.when(hi == query + 1)
        def _():
            part = bq // DIAG
            block(query * bq, [(n * part, (n + 1) * part, (n + 1) * part) for n in range(DIAG)], True)

        for n, kind in enumerate(kinds):

            @pl.when(item == n)
            def _():
                for i in range(hb):
                    if kind == "state":
                        outs[-1][0, i] = mix_s[i]
                        outs[-1][0, i, d + 1 : d + 2, :] = top_s[i : i + 1, :]
                        continue
                    got = (mix_s[i, :d, :] * (1 / mix_s[i, d : d + 1, :])).T.astype(jnp.bfloat16)
                    if kind == "out":
                        outs[n][:, i * d : (i + 1) * d] = got
                    else:
                        for to in (0, 1):

                            @pl.when(lax.rem(at[0], 2) ^ n == to)
                            def _():
                                outs[to][:, i * d : (i + 1) * d] = got

    if len(items) == 1:
        one_item(0)
    else:
        lax.fori_loop(0, len(items), lambda item, _: one_item(item), None)


def work(me, qkv, items, kinds, state=None, bq=512, hb=4):
    heads, tokens = qkv.shape[0] // 3, qkv.shape[1]
    n = heads // hb
    states = kinds.count("state")
    done = len(kinds) - states
    run = lambda i: pl.BlockSpec((hb, tokens, HEAD), lambda h, at: (i * n + h, 0, 0))
    specs = [run(0), run(1), run(2)]
    if state is not None:
        specs.append(pl.BlockSpec((1, hb, HEAD + 8, bq), lambda h, at: (0, h, 0, 0)))
    outs = [(pl.BlockSpec((bq, hb * HEAD), lambda h, at: (0, h)), jax.ShapeDtypeStruct((bq, heads * HEAD), jnp.bfloat16))] * done
    if states:
        outs.append((pl.BlockSpec((states, hb, HEAD + 8, bq), lambda h, at: (0, h, 0, 0)), jax.ShapeDtypeStruct((states, heads, HEAD + 8, bq), jnp.float32)))
    pairs = max(sum(i[c][2] - i[c][1] for i in items) for c in (0, 1))
    return pl.pallas_call(
        functools.partial(_work, items=items, kinds=kinds, scale=HEAD**-0.5, given=state is not None, bq=bq),
        grid_spec=pltpu.PrefetchScalarGridSpec(
            num_scalar_prefetch=1,
            grid=(n,),
            in_specs=specs,
            out_specs=[o[0] for o in outs],
            scratch_shapes=[pltpu.VMEM((hb, bq), jnp.float32), pltpu.VMEM((hb, HEAD + 8, bq), jnp.float32)],
        ),
        out_shape=[o[1] for o in outs],
        compiler_params=_params(),
        cost_estimate=pl.CostEstimate(flops=8 * pairs * heads * bq * bq * HEAD, bytes_accessed=4 * heads * tokens * HEAD, transcendentals=0),
    )(me, qkv, qkv, qkv, *([state] if state is not None else []))


def _output(at, *refs, count, last):
    sources, w_ref, rest = refs[:count], refs[count], refs[count + 1 :]
    o_ref, rows, sem = rest[-3:]
    core, depth = lax.rem(at[0], 2), sources[0].shape[1]

    @pl.when(pl.program_id(0) == 0)
    def _():
        for c in (0, 1):

            @pl.when(core == c)
            def _():
                for i in (0, 1):
                    to = rows.at[:, pl.ds((c ^ i) * depth, depth)]
                    pltpu.make_async_copy(sources[(2 * c + i) % count], to, sem.at[i]).start()

        for i in (0, 1):
            pltpu.make_async_copy(sources[i], rows.at[:, pl.ds(0, depth)], sem.at[i]).wait()

    total = jnp.dot(rows[...], w_ref[...], preferred_element_type=jnp.float32)
    if last:
        part_ref, x_ref = rest[:2]
        o_ref[...] = (x_ref[...].astype(jnp.float32) + (part_ref[...] + total)).astype(jnp.bfloat16)
    else:
        o_ref[...] = total


def output(me, sources, other, wo, part=None, x=None, bn=512):
    m, depth = sources[0].shape
    n = wo.shape[1]
    block = pl.BlockSpec((m, bn), lambda j, at: (0, j))
    last = part is not None
    return pl.pallas_call(
        functools.partial(_output, count=len(sources), last=last),
        grid_spec=pltpu.PrefetchScalarGridSpec(
            num_scalar_prefetch=1,
            grid=(n // bn,),
            in_specs=[HBM] * len(sources) + [pl.BlockSpec((2 * depth, bn), lambda j, at: (at[0] // 2 ^ other, j))] + ([block, block] if last else []),
            out_specs=block,
            scratch_shapes=[pltpu.VMEM((m, 2 * depth), jnp.bfloat16), pltpu.SemaphoreType.DMA((2,))],
        ),
        out_shape=jax.ShapeDtypeStruct((m, n), jnp.bfloat16 if last else jnp.float32),
        compiler_params=_params(),
        cost_estimate=pl.CostEstimate(flops=4 * m * depth * n, bytes_accessed=4 * depth * n, transcendentals=0),
    )(me, *sources, wo, *([part, x] if last else []))


def solution(mesh):
    n = mesh.shape["sp"]
    send = lambda t, *pairs: lax.ppermute(t, "sp", pairs)
    neighbours = ((0, 1), (1, 0), (2, 3), (3, 2))

    def step(x, gain, wq, wk, wv, wo):
        own, tokens = x.shape[0], x.shape[0] * n
        heads = wq.shape[1] // HEAD // n
        me = lax.axis_index("sp").astype(jnp.int32)[None]
        cos, sin = tables(tokens)

        def proj(pieces, place, block, kinds, into, bn=512):
            return project(me, pieces, place, block, cos, sin, (wq, wk, wv), kinds, into, tokens, heads, bn)

        a = norm(x, gain)
        near = send(a, *neighbours)
        zero = send(a, (0, 2), (2, 0))
        places = [[(0, 0), (1, own)], [(1, 0), (0, own)]]
        qkv = proj([a, near], places, lambda d: d // 2, (0, 1), None, 256)
        qkv, zero = lax.optimization_barrier((qkv, zero))
        one = send(lax.optimization_barrier((a, qkv))[0], (1, 3), (3, 1))
        zero_on = send(zero, *neighbours)
        qkv = proj([a, near], places, lambda d: d // 2, (2,), qkv, 256)
        places = [[(0, 0)], [(1, 0)]]
        qkv = proj([zero, zero_on], places, lambda d: (d // 2 ^ 1) * 2, (0, 1, 2), qkv)
        qkv, one = lax.optimization_barrier((qkv, one))
        one_on = send(one, *neighbours)
        x0, state = work(me, qkv, [((2, 0, 3, 0), (0, 0, 1, 0)), ((2, 0, 0, 0), (3, 2, 4, 0))], ["out", "state"])
        x0 = send(x0, (0, 2), (2, 0)), send(x0, (1, 2), (3, 0))
        qkv = proj([one_on, one], places, lambda d: (d // 2 ^ 1) * 2 + 1, (0, 1, 2), qkv)
        items = [((0, 0, 1, 0), (2, 0, 3, 0)), ((1, 0, 2, 0), (3, 0, 2, 1)), ((3, 0, 4, 0), (1, 0, 2, 0))]
        keep, give, x1 = work(me, qkv, items, ["core", "core", "out"], state)
        given = send(give, *neighbours)
        x1 = send(x1, (1, 3), (3, 1)), send(x1, (0, 3), (2, 1))
        part = output(me, (keep, given), 0, wo)
        return output(me, (*x0, *x1), 1, wo, part, x, 1024)

    tokens, whole = P(("dp", "sp"), None), P(None, None)
    step = jax.shard_map(step, mesh=mesh, in_specs=(tokens, P(None), whole, whole, whole, whole), out_specs=tokens, check_vma=False)
    return step
```

```python
import functools

import jax
import jax.numpy as jnp
from jax import lax
from jax.experimental import pallas as pl
from jax.experimental.pallas import tpu as pltpu

NEG = -1e30
HIDDEN = 2 * NEG
LOG2E = 1.4426950408889634


def _dot(a, b, ca, cb):
    return lax.dot_general(a, b, (((ca,), (cb,)), ((), ())), preferred_element_type=jnp.float32)


from jax.sharding import PartitionSpec as P

HEAD = 128
THETA = 10000
LIMIT = 34 * 2**20
DEPTHS = 2
DIAG = 2
HBM = pl.BlockSpec(memory_space=pl.ANY)


def _params(limit=LIMIT):
    return pltpu.CompilerParams(dimension_semantics=("arbitrary",), vmem_limit_bytes=limit)


def tables(tokens):
    half = HEAD // 2
    angle = jnp.arange(tokens, dtype=jnp.float32)[:, None] * THETA ** (-jnp.arange(half, dtype=jnp.float32) / half)
    cos, sin = jnp.cos(angle), jnp.sin(angle)
    return jnp.concatenate([cos, cos], -1), jnp.concatenate([-sin, sin], -1)


def _norm(x_ref, gain_ref, o_ref):
    wide = x_ref[...].astype(jnp.float32)
    scale = lax.rsqrt(jnp.mean(wide * wide, -1, keepdims=True) + 1e-6)
    o_ref[...] = (wide * scale * gain_ref[...][None].astype(jnp.float32)).astype(jnp.bfloat16)


def norm(x, gain, rows=128):
    m, d = x.shape
    block = pl.BlockSpec((rows, d), lambda i: (i, 0))
    return pl.pallas_call(
        _norm,
        grid=(m // rows,),
        in_specs=[block, pl.BlockSpec((d,), lambda i: (0,))],
        out_specs=block,
        out_shape=jax.ShapeDtypeStruct(x.shape, jnp.bfloat16),
        compiler_params=_params(60 * 2**20),
        cost_estimate=pl.CostEstimate(flops=5 * m * d, bytes_accessed=4 * m * d, transcendentals=0),
    )(x, gain)


def _project(at, *refs, count, place, kinds, bn, nb):
    pieces, (cos_ref, sin_ref), weights = refs[:count], refs[count : count + 2], refs[count + 2 : count + 2 + len(kinds)]
    out_ref, rows, buf, acc, sem, first_sem, row_sem = refs[-7:]
    step, heads = pl.program_id(0), bn // HEAD
    core, first = lax.rem(at[0], 2), at[0] * (nb * bn)
    m, steps = pieces[0].shape[0], len(kinds) * nb
    plain = kinds.index(2) * nb if 2 in kinds else steps
    deep = rows.shape[1] // DEPTHS

    def depth(c):
        return pl.ds(pl.multiple_of(c * deep, deep), deep)

    def start(s):
        for i, w in enumerate(weights):

            @pl.when((s >= i * nb) & (s < (i + 1) * nb))
            def _():
                columns = pl.ds(pl.multiple_of(first + (s - i * nb) * bn, bn), bn)
                pltpu.make_async_copy(w.at[:, columns], buf.at[lax.rem(s, 2)], sem.at[lax.rem(s, 2)]).start()

    def finish(got):
        for h in range(heads):
            t = got[:, h * HEAD : (h + 1) * HEAD].astype(jnp.float32)
            turned = t * cos_ref[...] + pltpu.roll(t, HEAD // 2, 1) * sin_ref[...]
            out_ref[h] = jnp.where(step < plain, turned, t).astype(jnp.bfloat16)

    @pl.when(step == 0)
    def _():
        columns = pl.ds(pl.multiple_of(first, bn), bn)
        for c in range(DEPTHS):
            for k in (0, 1):

                @pl.when(core == k)
                def _():
                    for p, to in place[k]:
                        pltpu.make_async_copy(pieces[p].at[:, depth(c)], rows.at[pl.ds(to, m), depth(c)], row_sem.at[c, to // m]).start()

            pltpu.make_async_copy(weights[0].at[depth(c), columns], buf.at[0, depth(c)], first_sem.at[c]).start()
        start(1)
        acc[...] = jnp.zeros_like(acc)

        def add(c, _):
            for i in range(rows.shape[0] // m):
                pltpu.make_async_copy(pieces[0].at[:, depth(c)], rows.at[pl.ds(i * m, m), depth(c)], row_sem.at[c, i]).wait()
            pltpu.make_async_copy(weights[0].at[depth(c), columns], buf.at[0, depth(c)], first_sem.at[c]).wait()
            acc[...] += jnp.dot(rows[:, depth(c)], buf[0, depth(c), :], preferred_element_type=jnp.float32)

        lax.fori_loop(0, DEPTHS, add, None)
        finish(acc[...].astype(jnp.bfloat16))

    @pl.when(step > 0)
    def _():
        slot = lax.rem(step, 2)

        @pl.when(step + 1 < steps)
        def _():
            start(step + 1)

        pltpu.make_async_copy(weights[0].at[:, pl.ds(0, bn)], buf.at[slot], sem.at[slot]).wait()
        finish(jnp.dot(rows[...], buf[slot], preferred_element_type=jnp.float32).astype(jnp.bfloat16))


def project(me, pieces, place, block, cos, sin, weights, kinds, into, tokens, heads, bn):
    m, d = pieces[0].shape
    nb = heads * HEAD // bn
    total = m * len(place[0])
    rows = pl.BlockSpec((total, HEAD), lambda s, at: (block(at[0]), 0))
    given = [*pieces, cos, sin, *(weights[k] for k in kinds)] + ([] if into is None else [into])
    specs = [HBM] * len(pieces) + [rows, rows] + [HBM] * (len(kinds) + (into is not None))
    return pl.pallas_call(
        functools.partial(_project, count=len(pieces), place=place, kinds=kinds, bn=bn, nb=nb),
        grid_spec=pltpu.PrefetchScalarGridSpec(
            num_scalar_prefetch=1,
            grid=(len(kinds) * nb,),
            in_specs=specs,
            out_specs=pl.BlockSpec((bn // HEAD, total, HEAD), lambda s, at: (s + kinds[0] * nb, block(at[0]), 0)),
            scratch_shapes=[
                pltpu.VMEM((total, d), jnp.bfloat16),
                pltpu.VMEM((2, d, bn), jnp.bfloat16),
                pltpu.VMEM((total, bn), jnp.float32),
                pltpu.SemaphoreType.DMA((2,)),
                pltpu.SemaphoreType.DMA((DEPTHS,)),
                pltpu.SemaphoreType.DMA((DEPTHS, len(place[0]))),
            ],
        ),
        out_shape=jax.ShapeDtypeStruct((3 * heads, tokens, HEAD), jnp.bfloat16),
        input_output_aliases={} if into is None else {len(given): 0},
        compiler_params=_params(),
        cost_estimate=pl.CostEstimate(flops=2 * len(kinds) * total * d * heads * HEAD, bytes_accessed=2 * len(kinds) * d * heads * HEAD, transcendentals=0),
    )(me, *given)


def _pick(at, items, i, field):
    got = [jnp.where(lax.div(at[0], 2) == 0, a[field], b[field]) for a, b in items]
    value = got[-1]
    for n in range(len(got) - 2, -1, -1):
        value = jnp.where(i == n, got[n], value)
    return value


def _work(at, q_ref, k_ref, v_ref, *rest, items, kinds, scale, given, bq):
    top_s, mix_s = rest[-2:]
    state_in, outs = (rest[0], rest[1:-2]) if given else (None, rest[:-2])
    hb, _, d = q_ref.shape
    e = scale * LOG2E

    def one_item(item):
        query, lo, hi, goes_on = (_pick(at, items, item, f) for f in range(4))

        @pl.when(goes_on == 0)
        def _():
            top_s[...] = jnp.full(top_s.shape, NEG, jnp.float32)
            mix_s[...] = jnp.zeros(mix_s.shape, jnp.float32)

        if given:

            @pl.when(goes_on == 1)
            def _():
                for i in range(hb):
                    top_s[i : i + 1, :] = state_in[0, i, d + 1 : d + 2, :]
                    mix_s[i] = state_in[0, i]

        def block(first, pieces, masked):
            pieces = [(i, slice(a, b), keys) for i in range(hb) for a, b, keys in pieces]
            here = lambda keys: pl.ds(pl.multiple_of(first, bq), keys)
            there = lambda cols: pl.ds(pl.multiple_of(query * bq + cols.start, cols.stop - cols.start), cols.stop - cols.start)
            scores = [_dot(k_ref[i, here(keys), :], q_ref[i, there(cols), :], 1, 1) for i, cols, keys in pieces]
            weights, keeps = [], []
            for (i, cols, _), s in zip(pieces, scores):
                if masked:
                    s = jnp.where(lax.broadcasted_iota(jnp.int32, s.shape, 1) + cols.start >= lax.broadcasted_iota(jnp.int32, s.shape, 0), s, HIDDEN)
                old = top_s[i : i + 1, cols]
                top = jnp.maximum(old, s.max(axis=0, keepdims=True))
                top_s[i : i + 1, cols] = top
                weights.append(jnp.exp2((s - top) * e).astype(jnp.bfloat16))
                keeps.append(jnp.exp2((old - top) * e))
            for (i, cols, keys), p, keep in zip(pieces, weights, keeps):
                values = jnp.concatenate([v_ref[i, here(keys), :].T, jnp.ones((8, keys), jnp.bfloat16)], axis=0)
                mix_s[i, :, cols] = mix_s[i, :, cols] * keep + _dot(values, p, 1, 0)

        lax.fori_loop(lo, jnp.minimum(hi, query), lambda j, _: block(j * bq, [(0, bq, bq)], False), None)

        @pl.when(hi == query + 1)
        def _():
            part = bq // DIAG
            block(query * bq, [(n * part, (n + 1) * part, (n + 1) * part) for n in range(DIAG)], True)

        for n, kind in enumerate(kinds):

            @pl.when(item == n)
            def _():
                for i in range(hb):
                    if kind == "state":
                        outs[-1][0, i] = mix_s[i]
                        outs[-1][0, i, d + 1 : d + 2, :] = top_s[i : i + 1, :]
                        continue
                    got = (mix_s[i, :d, :] * (1 / mix_s[i, d : d + 1, :])).T.astype(jnp.bfloat16)
                    if kind == "out":
                        outs[n][:, i * d : (i + 1) * d] = got
                    else:
                        for to in (0, 1):

                            @pl.when(lax.rem(at[0], 2) ^ n == to)
                            def _():
                                outs[to][:, i * d : (i + 1) * d] = got

    if len(items) == 1:
        one_item(0)
    else:
        lax.fori_loop(0, len(items), lambda item, _: one_item(item), None)


def work(me, qkv, items, kinds, state=None, bq=512, hb=4):
    heads, tokens = qkv.shape[0] // 3, qkv.shape[1]
    n = heads // hb
    states = kinds.count("state")
    done = len(kinds) - states
    run = lambda i: pl.BlockSpec((hb, tokens, HEAD), lambda h, at: (i * n + h, 0, 0))
    specs = [run(0), run(1), run(2)]
    if state is not None:
        specs.append(pl.BlockSpec((1, hb, HEAD + 8, bq), lambda h, at: (0, h, 0, 0)))
    outs = [(pl.BlockSpec((bq, hb * HEAD), lambda h, at: (0, h)), jax.ShapeDtypeStruct((bq, heads * HEAD), jnp.bfloat16))] * done
    if states:
        outs.append((pl.BlockSpec((states, hb, HEAD + 8, bq), lambda h, at: (0, h, 0, 0)), jax.ShapeDtypeStruct((states, heads, HEAD + 8, bq), jnp.float32)))
    pairs = max(sum(i[c][2] - i[c][1] for i in items) for c in (0, 1))
    return pl.pallas_call(
        functools.partial(_work, items=items, kinds=kinds, scale=HEAD**-0.5, given=state is not None, bq=bq),
        grid_spec=pltpu.PrefetchScalarGridSpec(
            num_scalar_prefetch=1,
            grid=(n,),
            in_specs=specs,
            out_specs=[o[0] for o in outs],
            scratch_shapes=[pltpu.VMEM((hb, bq), jnp.float32), pltpu.VMEM((hb, HEAD + 8, bq), jnp.float32)],
        ),
        out_shape=[o[1] for o in outs],
        compiler_params=_params(),
        cost_estimate=pl.CostEstimate(flops=8 * pairs * heads * bq * bq * HEAD, bytes_accessed=4 * heads * tokens * HEAD, transcendentals=0),
    )(me, qkv, qkv, qkv, *([state] if state is not None else []))


def _output(at, *refs, count, other, last):
    sources, w, rest = refs[:count], refs[count], refs[count + 1 :]
    o_ref, rows, buf, sem, row_sem = rest[-5:]
    core, chip, step, steps = lax.rem(at[0], 2), lax.div(at[0], 2) ^ other, pl.program_id(0), pl.num_programs(0)
    depth, bn = sources[0].shape[1], o_ref.shape[1]

    def copy(s):
        run = pl.ds(pl.multiple_of(chip * 2 * depth, 2 * depth), 2 * depth)
        columns = pl.ds(pl.multiple_of(s * bn, bn), bn)
        return pltpu.make_async_copy(w.at[run, columns], buf.at[lax.rem(s, 2)], sem.at[lax.rem(s, 2)])

    @pl.when(step == 0)
    def _():
        for c in (0, 1):

            @pl.when(core == c)
            def _():
                for i in (0, 1):
                    to = rows.at[:, pl.ds((c ^ i) * depth, depth)]
                    pltpu.make_async_copy(sources[(2 * c + i) % count], to, row_sem.at[i]).start()

        copy(0).start()
        for i in (0, 1):
            pltpu.make_async_copy(sources[i], rows.at[:, pl.ds(0, depth)], row_sem.at[i]).wait()

    copy(step).wait()

    @pl.when(step + 1 < steps)
    def _():
        copy(step + 1).start()

    total = jnp.dot(rows[...], buf[lax.rem(step, 2)], preferred_element_type=jnp.float32)
    if last:
        part_ref, x_ref = rest[:2]
        o_ref[...] = (x_ref[...].astype(jnp.float32) + (part_ref[...] + total)).astype(jnp.bfloat16)
    else:
        o_ref[...] = total


def output(me, sources, other, wo, part=None, x=None, bn=512):
    m, depth = sources[0].shape
    n = wo.shape[1]
    block = pl.BlockSpec((m, bn), lambda j, at: (0, j))
    last = part is not None
    return pl.pallas_call(
        functools.partial(_output, count=len(sources), other=other, last=last),
        grid_spec=pltpu.PrefetchScalarGridSpec(
            num_scalar_prefetch=1,
            grid=(n // bn,),
            in_specs=[HBM] * (len(sources) + 1) + ([block, block] if last else []),
            out_specs=block,
            scratch_shapes=[
                pltpu.VMEM((m, 2 * depth), jnp.bfloat16),
                pltpu.VMEM((2, 2 * depth, bn), jnp.bfloat16),
                pltpu.SemaphoreType.DMA((2,)),
                pltpu.SemaphoreType.DMA((2,)),
            ],
        ),
        out_shape=jax.ShapeDtypeStruct((m, n), jnp.bfloat16 if last else jnp.float32),
        compiler_params=_params(),
        cost_estimate=pl.CostEstimate(flops=4 * m * depth * n, bytes_accessed=4 * depth * n, transcendentals=0),
    )(me, *sources, wo, *([part, x] if last else []))


def solution(mesh):
    n = mesh.shape["sp"]
    send = lambda t, *pairs: lax.ppermute(t, "sp", pairs)
    neighbours = ((0, 1), (1, 0), (2, 3), (3, 2))

    def step(x, gain, wq, wk, wv, wo):
        own, tokens = x.shape[0], x.shape[0] * n
        heads = wq.shape[1] // HEAD // n
        me = lax.axis_index("sp").astype(jnp.int32)[None]
        cos, sin = tables(tokens)

        def proj(pieces, place, block, kinds, into, bn=512):
            return project(me, pieces, place, block, cos, sin, (wq, wk, wv), kinds, into, tokens, heads, bn)

        a = norm(x, gain)
        near = send(a, *neighbours)
        zero = send(a, (0, 2), (2, 0))
        places = [[(0, 0), (1, own)], [(1, 0), (0, own)]]
        qkv = proj([a, near], places, lambda d: d // 2, (0, 1), None, 256)
        qkv, zero = lax.optimization_barrier((qkv, zero))
        one = send(lax.optimization_barrier((a, qkv))[0], (1, 3), (3, 1))
        zero_on = send(zero, *neighbours)
        qkv = proj([a, near], places, lambda d: d // 2, (2,), qkv, 256)
        places = [[(0, 0)], [(1, 0)]]
        qkv = proj([zero, zero_on], places, lambda d: (d // 2 ^ 1) * 2, (0, 1, 2), qkv)
        qkv, one = lax.optimization_barrier((qkv, one))
        one_on = send(one, *neighbours)
        x0, state = work(me, qkv, [((2, 0, 3, 0), (0, 0, 1, 0)), ((2, 0, 0, 0), (3, 2, 4, 0))], ["out", "state"])
        x0 = send(x0, (0, 2), (2, 0)), send(x0, (1, 2), (3, 0))
        qkv = proj([one_on, one], places, lambda d: (d // 2 ^ 1) * 2 + 1, (0, 1, 2), qkv)
        items = [((0, 0, 1, 0), (2, 0, 3, 0)), ((1, 0, 2, 0), (3, 0, 2, 1)), ((3, 0, 4, 0), (1, 0, 2, 0))]
        keep, give, x1 = work(me, qkv, items, ["core", "core", "out"], state)
        given = send(give, *neighbours)
        x1 = send(x1, (1, 3), (3, 1)), send(x1, (0, 3), (2, 1))
        part = output(me, (keep, given), 0, wo)
        return output(me, (*x0, *x1), 1, wo, part, x, 1024)

    tokens, whole = P(("dp", "sp"), None), P(None, None)
    step = jax.shard_map(step, mesh=mesh, in_specs=(tokens, P(None), whole, whole, whole, whole), out_specs=tokens, check_vma=False)
    return step
```
